32 devices in a mesh: groups: 2 (over x), expert: 16 (over z, y, core).
Axes of the slice: x: 2, y: 2, z: 4, core: 2. Of those that a mesh axis runs over, the one named last changes fastest.
Arguments:
- tokens: bfloat16 [1024, 2048], P(('groups', 'expert')), parts along dimension 0, may hold values from -6 to 6
- expert_ids: int32 [1024, 2], P(('groups', 'expert')), parts along dimension 0, may hold values from 0 to 7, all different within a row; in each aligned block of 32 rows (0 to 31, 32 to 63, ...) at most 16 rows name the same one
- member_ids: int32 [1024], P(('groups', 'expert')), parts along dimension 0, may hold values from 0 to 7
- combine_weights: float32 [1024, 2], P(('groups', 'expert')), parts along dimension 0, may hold values from 0.25 to 1
- gate_weight: bfloat16 [2048, 57344], P(None, 'expert'), may hold values from -0.125 to 0.125
- up_weight: bfloat16 [2048, 57344], P(None, 'expert'), may hold values from -0.125 to 0.125
- down_weight: bfloat16 [57344, 2048], P('expert'), may hold values from -0.0625 to 0.0625
- input_factors: float32 [8, 8, 4096], replicated, may hold values from 0.5 to 2
- hidden_factors: float32 [8, 2, 57344], P(None, None, 'expert'), may hold values from 0.5 to 2
- output_factors: float32 [8, 8, 2048], replicated, may hold values from 0.5 to 2
Outputs:
- mixed: bfloat16 [1024, 2048], P(('groups', 'expert')), parts along dimension 0
The draws below stay inside these ranges and needn't reach their ends.
There are 2 independent parts, one for each index of `groups`. The reference program is written for one: setup_inputs(seed, part) draws one part's arguments, and reference() takes and returns one part's arrays. A program takes and returns all parts, laid end to end along the dimension named above; an argument that names none is the same for every part. Nothing has to cross between parts.
Inputs may be any that keep to these rules, and one draw needn't show every extreme that they name: `expert_ids`: the two experts of a token differ. Among the 32 tokens of one device no expert is named more than 16 times.
All inputs are finite; a program needn't handle non-finite values.
Results may differ from the reference program's by a relative error of at most 0.012.
Values may be sent and summed in bfloat16 or wider, within the bound.
No kernel may reach another device: no remote copies, remote signals or barrier semaphores. Data moves between devices by JAX's collectives and lax.ppermute only.
A program may use at most 128 MiB of HBM per device.

```python
import math
import jax
import jax.numpy as jnp
import numpy as np
from jax import lax

D = 2048
FF = 7168
EXPERTS = 8
MEMBERS = 8
TOK_DEV = 32
CAP = 16
SPLIT = 2
FF_DEV = 3584
TOKENS = 512


def set_ends(entries, stream_key, smallest, top_value):
    longest = entries.shape.index(max(entries.shape))
    spots = []
    for shift in (0, 1):
        where = [jax.random.randint(jax.random.fold_in(stream_key, axis), (), 0, length) for axis, length in enumerate(entries.shape)]
        where[longest] = (where[longest] + shift) % entries.shape[longest]
        spots.append(tuple(where))
    return entries.at[spots[0]].set(smallest).at[spots[1]].set(top_value)


def steps_of(key, shape, cuts, low, largest):
    def one(position, blocks):
        heights = jax.random.uniform(jax.random.fold_in(jax.random.fold_in(key, 6), position), (blocks,), jnp.float32, low / len(cuts), largest / len(cuts))
        return jnp.repeat(jnp.exp(heights), shape[position] // blocks).reshape((-1,) + (1,) * (len(shape) - position - 1))

    factor_of = one(*cuts[0])
    for cut in cuts[1:]:
        factor_of = factor_of * one(*cut)
    return factor_of


def deal_out(stream_key, own, number, rows, amount, top, bound, slope):
    order = jax.random.permutation(stream_key, amount)
    crowded, usual = load_shares(amount, rows * top, bound, slope, True), load_shares(amount, rows * top, bound, slope, False)
    places = jnp.arange(amount)

    def named(tallies, turn):
        used = int((tallies > 0).sum())
        fixed = max(1, used // 4)
        moved = fixed + (places - fixed + turn * (used - fixed)) % max(1, amount - fixed)
        return jnp.zeros((amount,), jnp.int32).at[order[jnp.where(places < fixed, places, moved)]].set(jnp.asarray(tallies, jnp.int32))

    tallies = jnp.where(number % 4 == 0, named(crowded, number // 4), named(usual, number - number // 4 - 1))
    mixed = jax.random.permutation(jax.random.fold_in(own, 3), amount)
    donor, receiver = mixed[0:amount // 2 * 2:2], mixed[1:amount // 2 * 2:2]
    room = jnp.minimum(tallies[donor] - 1, bound - tallies[receiver]) // 2
    room = jnp.where((donor == order[0]) | (receiver == order[0]) | (tallies[receiver] == 0), 0, jnp.maximum(room, 0))
    moved = jax.random.randint(jax.random.fold_in(own, 4), (amount // 2,), 0, 1 << 20) % (room + 1)
    tallies = tallies.at[donor].add(-moved).at[receiver].add(moved)
    items = jnp.searchsorted(jnp.cumsum(tallies), jnp.arange(rows * top), side="right").astype(jnp.int32)
    grid = items.reshape(top, rows).T
    grid = grid[jax.random.permutation(jax.random.fold_in(own, 1), rows)]
    turn = jax.random.randint(jax.random.fold_in(own, 2), (rows, 1), 0, top)
    return jnp.take_along_axis(grid, (jnp.arange(top)[None, :] + turn) % top, axis=1)


def load_shares(count, total, most, lean, full):
    portions = [(1 << 20) // math.isqrt(grade ** lean) + 1 for grade in range(1, count + 1)]
    largest = most if full else min(most, max(-(-total // count), total * portions[0] // sum(portions)))
    least = 1 if total - largest >= count - 1 else 0
    holding, spare = [largest] + [least] * (count - 1), total - largest - least * (count - 1)
    while spare > 0:
        movable = [i for i in range(1, count) if holding[i] < largest] or [i for i in range(1, count) if holding[i] < most]
        whole, left = sum([portions[i] for i in movable]), spare
        for i in movable:
            more = min(most - holding[i], max(1, left * portions[i] // whole), spare)
            holding[i] = holding[i] + more
            spare = spare - more
    return np.array(holding)


def gaussian(own_key, shape, deviation, reach, split=(), kind=jnp.bfloat16):
    values = jax.random.normal(own_key, shape, jnp.float32) * deviation
    if len(split) > 0:
        values = steps_of(own_key, shape, split, -0.22, 0.18) * values
    return jnp.clip(values, min=-reach, max=reach).astype(kind)


def setup_inputs(seed: int = 0, part: int = 0) -> dict:
    keys = jax.random.split(jax.random.key(seed), 11)
    part_keys = jax.random.split(jax.random.fold_in(keys[10], part), 11)
    tokens = gaussian(part_keys[0], (TOKENS, D), 1.0, 6.0, ((0, 16),))
    expert_ids_keys = jax.random.split(jax.random.fold_in(part_keys[1], 1), TOKENS // TOK_DEV)
    expert_ids_turns = jax.random.permutation(jax.random.fold_in(part_keys[1], 3), TOKENS // TOK_DEV)
    expert_ids = jax.vmap(lambda own, number: deal_out(jax.random.fold_in(part_keys[1], 2), own, number, TOK_DEV, EXPERTS, 2, CAP, 2))(expert_ids_keys, expert_ids_turns).reshape((TOKENS, 2))
    member_ids = set_ends(jax.random.randint(part_keys[2], (TOKENS,), 0, MEMBERS), jax.random.fold_in(part_keys[2], 1), 0, MEMBERS - 1).astype(jnp.int32)
    combine_weights = jnp.clip(0.25 + 0.75 * jax.random.uniform(part_keys[3], (TOKENS, 2), jnp.float32) ** steps_of(part_keys[3], (TOKENS, 2), ((0, 16),), -0.2, 0.2), 0.25, 1.0)
    gate_weight = gaussian(keys[4], (D, EXPERTS * FF), D ** -0.5, 0.125, ((1, 16),))
    up_weight = gaussian(keys[5], (D, EXPERTS * FF), D ** -0.5, 0.125, ((1, 16),))
    down_weight = gaussian(keys[6], (EXPERTS * FF, D), FF ** -0.5, 0.0625, ((0, 16),))
    input_factors = jnp.clip(jnp.exp(jax.random.uniform(keys[7], (EXPERTS, MEMBERS, 2 * D), jnp.float32, math.log(0.5), math.log(2.0))), 0.5, 2.0)
    hidden_factors = jnp.clip(jnp.exp(math.log(2.0) - 1.3862944 * jax.random.uniform(keys[8], (MEMBERS, 2, EXPERTS * FF), jnp.float32) ** steps_of(keys[8], (MEMBERS, 2, EXPERTS * FF), ((2, 16),), -0.2, 0.2)), 0.5, 2.0)
    output_factors = jnp.clip(jnp.exp(jax.random.uniform(keys[9], (EXPERTS, MEMBERS, D), jnp.float32, math.log(0.5), math.log(2.0))), 0.5, 2.0)
    return {"tokens": tokens, "expert_ids": expert_ids, "member_ids": member_ids, "combine_weights": combine_weights, "gate_weight": gate_weight, "up_weight": up_weight, "down_weight": down_weight, "input_factors": input_factors, "hidden_factors": hidden_factors, "output_factors": output_factors}


def reference(tokens, expert_ids, member_ids, combine_weights, gate_weight, up_weight, down_weight, input_factors, hidden_factors, output_factors):
    pair_total = TOKENS * 2
    flat_expert = expert_ids.reshape(-1).astype(jnp.int32)
    ranking = jnp.argsort(flat_expert, stable=True).astype(jnp.int32)
    hits = (flat_expert[:, None] == jnp.arange(EXPERTS, dtype=jnp.int32)[None, :]).astype(jnp.int32)
    counts = jnp.sum(hits, 0).astype(jnp.int32)
    starts = (jnp.cumsum(counts) - counts).astype(jnp.int32)
    flat_weight = combine_weights.reshape(-1)
    block_rows = min(128, pair_total)
    total = jnp.zeros((TOKENS, D), jnp.float32)
    for expert_index in range(EXPERTS):
        low = expert_index * FF
        high = (expert_index + 1) * FF
        gate_cols = gate_weight[:, low:high]
        up_cols = up_weight[:, low:high]
        down_rows = down_weight[low:high].astype(jnp.float32).reshape(SPLIT, FF_DEV, D)
        in_table = input_factors[expert_index]
        out_table = output_factors[expert_index]
        first = starts[expert_index]
        number = counts[expert_index]

        def one_block(step_index, acc):
            local = step_index * block_rows + jnp.arange(block_rows, dtype=jnp.int32)
            valid = local < number
            picked = ranking[jnp.clip(first + local, 0, pair_total - 1)]
            token_index = picked // 2
            member = member_ids[token_index]
            row_data = tokens[token_index]
            in_scale = in_table[member]
            gate_in = (row_data * in_scale[:, :D]).astype(jnp.bfloat16)
            up_in = (row_data * in_scale[:, D:]).astype(jnp.bfloat16)
            gate = jnp.dot(gate_in, gate_cols, preferred_element_type=jnp.float32) * hidden_factors[member, 0, low:high]
            up = jnp.dot(up_in, up_cols, preferred_element_type=jnp.float32) * hidden_factors[member, 1, low:high]
            hidden = (jax.nn.silu(gate) * up).astype(jnp.bfloat16)
            pieces = jnp.einsum("rsf,sfd->rsd", hidden.astype(jnp.float32).reshape(block_rows, SPLIT, FF_DEV), down_rows)
            pieces = pieces.astype(jnp.bfloat16)
            result = jnp.sum(pieces.astype(jnp.float32), 1) * out_table[member]
            scale = jnp.where(valid, flat_weight[picked], jnp.zeros((), flat_weight.dtype))
            return acc.at[token_index].add(scale[:, None] * result)

        block_count = (number + block_rows - 1) // block_rows
        total = lax.fori_loop(jnp.zeros((), jnp.int32), block_count, one_block, total)
    return total.astype(jnp.bfloat16)
```

```python
import functools

import jax
import jax.numpy as jnp
from jax import lax
from jax.experimental import pallas as pl
from jax.experimental.pallas import tpu as pltpu
from jax.sharding import Mesh, PartitionSpec as P

EXPERTS = 8
MEMBERS = 8
CAP = 16
LANES = 128


def thirds(table):
    high = table.astype(jnp.bfloat16)
    rest = table - high.astype(jnp.float32)
    middle = rest.astype(jnp.bfloat16)
    low = (rest - middle.astype(jnp.float32)).astype(jnp.bfloat16)
    return jnp.concatenate([high, middle, low], axis=0)


def flag(condition):
    return jnp.where(condition, 1.0, 0.0)


def placing(ids):
    tok_count = ids.shape[1]
    slots = EXPERTS * CAP
    row = lax.broadcasted_iota(jnp.int32, (slots, tok_count), 0)
    expert = row // CAP
    first = ids[0:1, :] == expert
    second = ids[1:2, :] == expert
    named = flag(first) + flag(second)
    before = flag(
        lax.broadcasted_iota(jnp.int32, (tok_count, tok_count), 0)
        < lax.broadcasted_iota(jnp.int32, (tok_count, tok_count), 1)
    ).astype(jnp.bfloat16)
    rank = jnp.dot(named.astype(jnp.bfloat16), before, preferred_element_type=jnp.float32)
    here = rank == (row % CAP).astype(jnp.float32)
    return flag(first & here), flag(second & here)


def pack_kernel(tokens, ids, member_ids, rows):
    width = tokens.shape[1]
    first, second = placing(ids[...])
    chosen = first + second
    rows[:, :width] = jnp.dot(
        chosen.astype(jnp.bfloat16), tokens[...], preferred_element_type=jnp.float32
    ).astype(jnp.bfloat16)
    plus = (member_ids[...] + 1).astype(jnp.float32)
    member = jnp.sum(chosen * plus, axis=1, keepdims=True)
    rows[:, width:] = jnp.broadcast_to(member, (rows.shape[0], LANES)).astype(jnp.bfloat16)


def ffn_kernel(
    own_expert, rows, in_factors, hid_factors, gate_weight, up_weight, down_weight, partial_out,
    gate_in, up_in, select, total,
):
    step = pl.program_id(0)
    members = in_factors.shape[1]
    width = gate_in.shape[1]
    count = rows.shape[0]

    @pl.when(step == 0)
    def _():
        member = rows[:, width:width + 1].astype(jnp.float32) - 1.0
        column = lax.broadcasted_iota(jnp.int32, (count, 3 * members), 1) % members
        chosen = flag(member == column.astype(jnp.float32)).astype(jnp.bfloat16)
        select[...] = chosen
        scale = jnp.dot(chosen, thirds(in_factors[0]), preferred_element_type=jnp.float32)
        data = rows[:, :width].astype(jnp.float32)
        gate_in[...] = (data * scale[:, :width]).astype(jnp.bfloat16)
        up_in[...] = (data * scale[:, width:]).astype(jnp.bfloat16)

    chosen = select[...]
    gate_scale = jnp.dot(chosen, thirds(hid_factors[0]), preferred_element_type=jnp.float32)
    up_scale = jnp.dot(chosen, thirds(hid_factors[1]), preferred_element_type=jnp.float32)
    gate = jnp.dot(gate_in[...], gate_weight[...], preferred_element_type=jnp.float32) * gate_scale
    up = jnp.dot(up_in[...], up_weight[...], preferred_element_type=jnp.float32) * up_scale
    hidden = (gate / (1.0 + jnp.exp(-gate)) * up).astype(jnp.bfloat16)
    part = jnp.dot(hidden, down_weight[...], preferred_element_type=jnp.float32)

    @pl.when(step == 0)
    def _():
        total[...] = part

    @pl.when(step > 0)
    def _():
        total[...] = total[...] + part

    @pl.when(step == pl.num_programs(0) - 1)
    def _():
        partial_out[...] = total[...].astype(jnp.bfloat16)


def combine_kernel(summed, ids, member_ids, weights, out_factors, mixed):
    tok_count = ids.shape[1]
    table = thirds(out_factors[...])
    entries = out_factors.shape[0]
    spot = lax.broadcasted_iota(jnp.int32, (3 * entries, tok_count), 0) % entries
    diagonal = lax.broadcasted_iota(jnp.int32, (tok_count, tok_count), 0) == (
        lax.broadcasted_iota(jnp.int32, (tok_count, tok_count), 1)
    )
    over_rows = (((0,), (0,)), ((), ()))
    result = None
    for route, place in enumerate(placing(ids[...])):
        picked = lax.dot_general(
            place.astype(jnp.bfloat16), summed[...], over_rows, preferred_element_type=jnp.float32
        )
        entry = ids[route:route + 1, :] * MEMBERS + member_ids[...]
        chosen = flag(spot == entry).astype(jnp.bfloat16)
        scale = lax.dot_general(chosen, table, over_rows, preferred_element_type=jnp.float32)
        weight = jnp.sum(
            jnp.where(diagonal, weights[route:route + 1, :], 0.0), axis=1, keepdims=True
        )
        term = picked * scale * weight
        result = term if result is None else result + term
    mixed[...] = result.astype(jnp.bfloat16)


def block_of(units):
    best = LANES
    for block in range(LANES, 513, LANES):
        if units % block == 0:
            best = block
    return best


def run_rows(
    rows, own_expert, gate_weight, up_weight, down_weight, input_factors, hidden_factors
):
    count = rows.shape[0]
    width, units = gate_weight.shape
    members = input_factors.shape[1]
    block = block_of(units)
    spec = pltpu.PrefetchScalarGridSpec(
        num_scalar_prefetch=1,
        grid=(units // block,),
        in_specs=[
            pl.BlockSpec((count, rows.shape[1]), lambda i, own: (0, 0)),
            pl.BlockSpec((1, members, 2 * width), lambda i, own: (own[0], 0, 0)),
            pl.BlockSpec((2, members, block), lambda i, own: (0, 0, i)),
            pl.BlockSpec((width, block), lambda i, own: (0, i)),
            pl.BlockSpec((width, block), lambda i, own: (0, i)),
            pl.BlockSpec((block, width), lambda i, own: (i, 0)),
        ],
        out_specs=pl.BlockSpec((count, width), lambda i, own: (0, 0)),
        scratch_shapes=[
            pltpu.VMEM((count, width), jnp.bfloat16),
            pltpu.VMEM((count, width), jnp.bfloat16),
            pltpu.VMEM((count, 3 * members), jnp.bfloat16),
            pltpu.VMEM((count, width), jnp.float32),
        ],
    )
    return pl.pallas_call(
        ffn_kernel,
        grid_spec=spec,
        out_shape=jax.ShapeDtypeStruct((count, width), jnp.bfloat16),
        compiler_params=pltpu.CompilerParams(dimension_semantics=("arbitrary",)),
        name="ffn",
    )(
        own_expert, rows, input_factors, hidden_factors.transpose(1, 0, 2),
        gate_weight, up_weight, down_weight,
    )


def swapped(block, apart):
    count = lax.axis_size("share")
    route = [(place, place ^ apart) for place in range(count)]
    return lax.ppermute(block, "share", route)


def per_device(
    tokens,
    expert_ids,
    member_ids,
    combine_weights,
    gate_weight,
    up_weight,
    down_weight,
    input_factors,
    hidden_factors,
    output_factors,
):
    split = lax.axis_size("share")
    own_expert = lax.axis_index("owner").astype(jnp.int32).reshape(1)
    tok_count, width = tokens.shape
    slots = EXPERTS * CAP
    ids = expert_ids.T
    members = member_ids.reshape(1, tok_count)
    rows = pl.pallas_call(
        pack_kernel,
        out_shape=jax.ShapeDtypeStruct((slots, width + LANES), jnp.bfloat16),
        name="pack",
    )(tokens, ids, members)
    held = lax.all_to_all(
        rows.reshape(EXPERTS, CAP, width + LANES), "owner", split_axis=0, concat_axis=0, tiled=True
    ).reshape(slots, width + LANES)
    levels = split.bit_length() - 1
    for level in range(levels):
        held = jnp.concatenate([held, swapped(held, 1 << level)], axis=0)
    held = run_rows(
        held, own_expert, gate_weight, up_weight, down_weight, input_factors, hidden_factors
    )
    for level in reversed(range(levels)):
        half = held.shape[0] // 2
        other = swapped(held[half:], 1 << level)
        held = (held[:half].astype(jnp.float32) + other.astype(jnp.float32)).astype(jnp.bfloat16)
    summed = lax.all_to_all(
        held.reshape(EXPERTS, CAP, width), "owner", split_axis=0, concat_axis=0, tiled=True
    ).reshape(slots, width)
    return pl.pallas_call(
        combine_kernel,
        out_shape=jax.ShapeDtypeStruct((tok_count, width), jnp.bfloat16),
        name="combine",
    )(summed, ids, members, combine_weights.T, output_factors.reshape(EXPERTS * MEMBERS, width))


def solution(mesh):
    groups = mesh.shape["groups"]
    fine = Mesh(mesh.devices.reshape(groups, EXPERTS, -1), ("groups", "owner", "share"))
    expert = ("owner", "share")
    everyone = ("groups", "owner", "share")
    in_specs = (
        P(everyone, None),
        P(everyone, None),
        P(everyone),
        P(everyone, None),
        P(None, expert),
        P(None, expert),
        P(expert, None),
        P(),
        P(None, None, expert),
        P(),
    )
    return jax.shard_map(
        per_device, mesh=fine, in_specs=in_specs, out_specs=P(everyone, None), check_vma=False
    )
```

```python
import functools

import jax
import jax.numpy as jnp
from jax import lax
from jax.experimental import pallas as pl
from jax.experimental.pallas import tpu as pltpu
from jax.sharding import Mesh, PartitionSpec as P

EXPERTS = 8
MEMBERS = 8
CAP = 16
LANES = 128
VMEM_SPARE = 3 << 20
SLOTS = 3
CHUNKS = 4


def thirds(table):
    high = table.astype(jnp.bfloat16)
    rest = table - high.astype(jnp.float32)
    middle = rest.astype(jnp.bfloat16)
    low = (rest - middle.astype(jnp.float32)).astype(jnp.bfloat16)
    return jnp.concatenate([high, middle, low], axis=0)


def flag(condition):
    return jnp.where(condition, 1.0, 0.0)


def placing(ids):
    tok_count = ids.shape[1]
    slots = EXPERTS * CAP
    row = lax.broadcasted_iota(jnp.int32, (slots, tok_count), 0)
    expert = (row // CAP) ^ lax.axis_index("owner")
    first = ids[0:1, :] == expert
    second = ids[1:2, :] == expert
    named = flag(first) + flag(second)
    before = flag(
        lax.broadcasted_iota(jnp.int32, (tok_count, tok_count), 0)
        < lax.broadcasted_iota(jnp.int32, (tok_count, tok_count), 1)
    ).astype(jnp.bfloat16)
    rank = jnp.dot(named.astype(jnp.bfloat16), before, preferred_element_type=jnp.float32)
    here = rank == (row % CAP).astype(jnp.float32)
    return flag(first & here), flag(second & here)


def pack_kernel(tokens, ids, member_ids, *blocks):
    width = tokens.shape[1]
    first, second = placing(ids[...])
    chosen = first + second
    rows = jnp.dot(
        chosen.astype(jnp.bfloat16), tokens[...], preferred_element_type=jnp.float32
    ).astype(jnp.bfloat16)
    plus = (member_ids[...] + 1).astype(jnp.float32)
    member = jnp.sum(chosen * plus, axis=1, keepdims=True)
    member = jnp.broadcast_to(member, (rows.shape[0], LANES)).astype(jnp.bfloat16)
    for spot, block in enumerate(blocks):
        block[:, :width] = rows[spot * CAP:(spot + 1) * CAP]
        block[:, width:] = member[spot * CAP:(spot + 1) * CAP]


def ffn_kernel(in_factors, hid_factors, gate_weight, up_weight, down_weight, *refs):
    rows, gate_in, up_in, select, total, down_here, arrived = refs[-7:]
    count, width = gate_in.shape
    results, parts, low = [], list(refs[:-7]), 0
    while low < count:
        results.insert(0, parts.pop())
        low += results[0].shape[0]
    members = in_factors.shape[1]
    units = gate_weight.shape[1]
    block = block_of(units)
    steps = units // block

    def arrival(step):
        here = pl.ds(pl.multiple_of(step * block, block), block)
        slot = step % SLOTS
        return pltpu.make_async_copy(down_weight.at[here], down_here.at[slot], arrived.at[slot])

    for step in range(min(SLOTS - 1, steps)):
        arrival(step).start()
    low = 0
    for part in parts:
        rows[pl.ds(low, part.shape[0]), :] = part[...]
        low += part.shape[0]
    member = rows[:, width:width + 1].astype(jnp.float32) - 1.0
    column = lax.broadcasted_iota(jnp.int32, (count, 3 * members), 1) % members
    chosen = flag(member == column.astype(jnp.float32)).astype(jnp.bfloat16)
    select[...] = chosen
    owner = lax.axis_index("owner")
    slab = block_of(width)
    for low in range(0, width, slab):
        here = pl.ds(low, slab)
        data = rows[:, here].astype(jnp.float32)
        for offset, result in ((0, gate_in), (width, up_in)):
            table = thirds(in_factors[owner, :, pl.ds(offset + low, slab)])
            scale = jnp.dot(chosen, table, preferred_element_type=jnp.float32)
            result[:, here] = (data * scale).astype(jnp.bfloat16)

    def one_block(step, first):
        @pl.when(step + SLOTS - 1 < steps)
        def _():
            arrival(step + SLOTS - 1).start()

        here = pl.ds(pl.multiple_of(step * block, block), block)
        chosen = select[...]
        gate_table = thirds(hid_factors[:, 0, here])
        up_table = thirds(hid_factors[:, 1, here])
        gate_scale = jnp.dot(chosen, gate_table, preferred_element_type=jnp.float32)
        up_scale = jnp.dot(chosen, up_table, preferred_element_type=jnp.float32)
        gate = jnp.dot(gate_in[...], gate_weight[:, here], preferred_element_type=jnp.float32)
        up = jnp.dot(up_in[...], up_weight[:, here], preferred_element_type=jnp.float32)
        gate = gate * gate_scale
        hidden = (gate / (1.0 + jnp.exp(-gate)) * (up * up_scale)).astype(jnp.bfloat16)
        arrival(step).wait()
        part = jnp.dot(hidden, down_here[step % SLOTS], preferred_element_type=jnp.float32)
        total[...] = part if first else total[...] + part

    one_block(0, True)

    def body(step, carry):
        one_block(step, False)
        return carry

    lax.fori_loop(1, steps, body, 0)
    low = 0
    for result in results:
        result[...] = total[pl.ds(low, result.shape[0]), :].astype(jnp.bfloat16)
        low += result.shape[0]


def add_kernel(mine, other, *blocks):
    for spot, block in enumerate(blocks):
        here = pl.ds(spot * CAP, CAP)
        both = mine[here, :].astype(jnp.float32) + other[here, :].astype(jnp.float32)
        block[...] = both.astype(jnp.bfloat16)


def combine_kernel(ids, member_ids, weights, out_factors, *refs):
    mixed, summed = refs[-2:]
    for spot, block in enumerate(refs[:-2]):
        summed[pl.ds(spot * CAP, CAP), :] = block[...]
    tok_count = ids.shape[1]
    table = thirds(out_factors[...])
    entries = out_factors.shape[0]
    spot = lax.broadcasted_iota(jnp.int32, (3 * entries, tok_count), 0) % entries
    diagonal = lax.broadcasted_iota(jnp.int32, (tok_count, tok_count), 0) == (
        lax.broadcasted_iota(jnp.int32, (tok_count, tok_count), 1)
    )
    over_rows = (((0,), (0,)), ((), ()))
    result = None
    for route, place in enumerate(placing(ids[...])):
        picked = lax.dot_general(
            place.astype(jnp.bfloat16), summed[...], over_rows, preferred_element_type=jnp.float32
        )
        entry = ids[route:route + 1, :] * MEMBERS + member_ids[...]
        chosen = flag(spot == entry).astype(jnp.bfloat16)
        scale = lax.dot_general(chosen, table, over_rows, preferred_element_type=jnp.float32)
        weight = jnp.sum(
            jnp.where(diagonal, weights[route:route + 1, :], 0.0), axis=1, keepdims=True
        )
        term = picked * scale * weight
        result = term if result is None else result + term
    mixed[...] = result.astype(jnp.bfloat16)


def block_of(units):
    best = LANES
    for block in range(LANES, 513, LANES):
        if units % block == 0:
            best = block
    return best


def fetch_kernel(*refs):
    half = len(refs) // 2
    sources, results, arrived = refs[:half], refs[half:-1], refs[-1]
    copies = []
    for source, result in zip(sources, results):
        rows = source.shape[0] // CHUNKS
        for chunk in range(CHUNKS):
            part = pl.ds(chunk * rows, rows)
            copies.append(
                pltpu.make_async_copy(source.at[part], result.at[part], arrived.at[len(copies)])
            )
    for copy in copies:
        copy.start()
    for copy in copies:
        copy.wait()


def fetched(weights):
    vmem = pl.BlockSpec(memory_space=pltpu.VMEM)
    size = sum(weight.size * weight.dtype.itemsize for weight in weights)
    return pl.pallas_call(
        fetch_kernel,
        in_specs=[pl.BlockSpec(memory_space=pltpu.HBM)] * len(weights),
        out_specs=[vmem] * len(weights),
        out_shape=[jax.ShapeDtypeStruct(weight.shape, weight.dtype) for weight in weights],
        scratch_shapes=[pltpu.SemaphoreType.DMA((CHUNKS * len(weights),))],
        compiler_params=pltpu.CompilerParams(vmem_limit_bytes=5 * size // 8),
        cost_estimate=pl.CostEstimate(
            flops=512 * size, bytes_accessed=size, transcendentals=0
        ),
        name="fetch",
    )(*weights)


def run_rows(parts, sizes, gate_weight, up_weight, down_weight, input_factors, hidden_factors):
    count = sum(sizes)
    width, units = gate_weight.shape
    block = block_of(units)
    members = input_factors.shape[1]
    vmem = pl.BlockSpec(memory_space=pltpu.VMEM)
    hbm = pl.BlockSpec(memory_space=pltpu.HBM)
    return pl.pallas_call(
        ffn_kernel,
        in_specs=[vmem] * 4 + [hbm] + [vmem] * len(parts),
        out_specs=[vmem] * len(sizes),
        out_shape=[jax.ShapeDtypeStruct((size, width), jnp.bfloat16) for size in sizes],
        scratch_shapes=[
            pltpu.VMEM((count, width + LANES), jnp.bfloat16),
            pltpu.VMEM((count, width), jnp.bfloat16),
            pltpu.VMEM((count, width), jnp.bfloat16),
            pltpu.VMEM((count, 3 * members), jnp.bfloat16),
            pltpu.VMEM((count, width), jnp.float32),
            pltpu.VMEM((SLOTS, block, width), jnp.bfloat16),
            pltpu.SemaphoreType.DMA((SLOTS,)),
        ],
        compiler_params=pltpu.CompilerParams(
            vmem_limit_bytes=(2 * SLOTS * block + 11 * count) * width + VMEM_SPARE
        ),
        name="ffn",
    )(input_factors, hidden_factors, gate_weight, up_weight, down_weight, *parts)


def swapped(block, axis, apart):
    route = [(place, place ^ apart) for place in range(lax.axis_size(axis))]
    return lax.ppermute(block, axis, route)


def per_device(
    tokens,
    expert_ids,
    member_ids,
    combine_weights,
    gate_weight,
    up_weight,
    down_weight,
    input_factors,
    hidden_factors,
    output_factors,
):
    split = lax.axis_size("share")
    levels = split.bit_length() - 1
    tok_count, width = tokens.shape
    slots = EXPERTS * CAP
    ids = expert_ids.T
    members = member_ids.reshape(1, tok_count)
    small = pltpu.CompilerParams(vmem_limit_bytes=VMEM_SPARE)
    blocks = pl.pallas_call(
        pack_kernel,
        out_shape=[jax.ShapeDtypeStruct((CAP, width + LANES), jnp.bfloat16)] * EXPERTS,
        compiler_params=small,
        name="pack",
    )(tokens, ids, members)
    *blocks, gate_weight, up_weight = lax.optimization_barrier((*blocks, gate_weight, up_weight))
    arrived = [
        swapped(block, "owner", apart) if apart else block for apart, block in enumerate(blocks)
    ]
    *arrived, gate_weight, up_weight = lax.optimization_barrier(
        (*arrived, *fetched((gate_weight, up_weight)))
    )
    groups = [[] for _ in range(levels + 1)]
    for block in arrived:
        held = [block]
        for level in range(levels):
            give = held[0] if level == 0 else jnp.concatenate(held, axis=0)
            held.append(swapped(give, "share", 1 << level))
        for group, part in zip(groups, held):
            group.append(part)
    parts = [part for group in groups for part in group]
    sizes = [sum(part.shape[0] for part in group) for group in groups]
    results = list(run_rows(
            parts, sizes, gate_weight, up_weight, down_weight, input_factors, hidden_factors
        ))
    for level in reversed(range(1, levels)):
        other = swapped(results.pop(), "share", 1 << level).reshape(EXPERTS, -1, width)
        low = 0
        for spot, mine in enumerate(results):
            rows = mine.shape[0] // EXPERTS
            theirs = other[:, low:low + rows].reshape(mine.shape)
            both = mine.astype(jnp.float32) + theirs.astype(jnp.float32)
            results[spot] = both.astype(jnp.bfloat16)
            low += rows
    blocks = pl.pallas_call(
        add_kernel,
        out_shape=[jax.ShapeDtypeStruct((CAP, width), jnp.bfloat16)] * EXPERTS,
        compiler_params=small,
        name="add",
    )(results[0], swapped(results[1], "share", 1))
    returned = [
        swapped(block, "owner", apart) if apart else block for apart, block in enumerate(blocks)
    ]
    return pl.pallas_call(
        combine_kernel,
        out_shape=jax.ShapeDtypeStruct((tok_count, width), jnp.bfloat16),
        scratch_shapes=[pltpu.VMEM((slots, width), jnp.bfloat16)],
        compiler_params=small,
        name="combine",
    )(
        ids, members, combine_weights.T,
        output_factors.reshape(EXPERTS * MEMBERS, width), *returned,
    )


def solution(mesh):
    groups = mesh.shape["groups"]
    fine = Mesh(mesh.devices.reshape(groups, EXPERTS, -1), ("groups", "owner", "share"))
    expert = ("owner", "share")
    everyone = ("groups", "owner", "share")
    in_specs = (
        P(everyone, None),
        P(everyone, None),
        P(everyone),
        P(everyone, None),
        P(None, expert),
        P(None, expert),
        P(expert, None),
        P(),
        P(None, None, expert),
        P(),
    )
    return jax.shard_map(
        per_device, mesh=fine, in_specs=in_specs, out_specs=P(everyone, None), check_vma=False
    )
```

```python
import functools

import jax
import jax.numpy as jnp
from jax import lax
from jax.experimental import pallas as pl
from jax.experimental.pallas import tpu as pltpu
from jax.sharding import Mesh, PartitionSpec as P

EXPERTS = 8
MEMBERS = 8
CAP = 16
LANES = 128
VMEM_SPARE = 3 << 20
VMEM_LARGE = 34 << 20
SLOTS = 3
CHUNKS = 4


def thirds(table):
    high = table.astype(jnp.bfloat16)
    rest = table - high.astype(jnp.float32)
    middle = rest.astype(jnp.bfloat16)
    low = (rest - middle.astype(jnp.float32)).astype(jnp.bfloat16)
    return jnp.concatenate([high, middle, low], axis=0)


def flag(condition):
    return jnp.where(condition, 1.0, 0.0)


def placing(ids):
    tok_count = ids.shape[1]
    slots = EXPERTS * CAP
    row = lax.broadcasted_iota(jnp.int32, (slots, tok_count), 0)
    expert = (EXPERTS - 1 - row // CAP) ^ lax.axis_index("owner")
    first = ids[0:1, :] == expert
    second = ids[1:2, :] == expert
    named = flag(first) + flag(second)
    before = flag(
        lax.broadcasted_iota(jnp.int32, (tok_count, tok_count), 0)
        < lax.broadcasted_iota(jnp.int32, (tok_count, tok_count), 1)
    ).astype(jnp.bfloat16)
    rank = jnp.dot(named.astype(jnp.bfloat16), before, preferred_element_type=jnp.float32)
    here = rank == (row % CAP).astype(jnp.float32)
    return flag(first & here), flag(second & here)


def pack_kernel(tokens, ids, member_ids, *blocks):
    width = tokens.shape[1]
    first, second = placing(ids[...])
    chosen = first + second
    rows = jnp.dot(
        chosen.astype(jnp.bfloat16), tokens[...], preferred_element_type=jnp.float32
    ).astype(jnp.bfloat16)
    plus = (member_ids[...] + 1).astype(jnp.float32)
    member = jnp.sum(chosen * plus, axis=1, keepdims=True)
    member = jnp.broadcast_to(member, (rows.shape[0], LANES)).astype(jnp.bfloat16)
    for spot, block in enumerate(blocks):
        block[:, :width] = rows[spot * CAP:(spot + 1) * CAP]
        block[:, width:] = member[spot * CAP:(spot + 1) * CAP]


def ffn_kernel(in_factors, hid_factors, gate_weight, up_weight, down_weight, *refs):
    rows, gate_in, up_in, select, total, up_here, down_here, arrived = refs[-8:]
    count, width = gate_in.shape
    results, parts, low = [], list(refs[:-8]), 0
    while low < count:
        results.insert(0, parts.pop())
        low += results[0].shape[0]
    members = in_factors.shape[1]
    units = gate_weight.shape[1]
    block = block_of(units)
    steps = units // block

    def arrivals(step):
        here = pl.ds(pl.multiple_of(step * block, block), block)
        slot = step % SLOTS
        return (
            pltpu.make_async_copy(up_weight.at[:, here], up_here.at[slot], arrived.at[0, slot]),
            pltpu.make_async_copy(down_weight.at[here], down_here.at[slot], arrived.at[1, slot]),
        )

    for step in range(min(SLOTS - 1, steps)):
        for copy in arrivals(step):
            copy.start()
    low = 0
    for part in parts:
        rows[pl.ds(low, part.shape[0]), :] = part[...]
        low += part.shape[0]
    member = rows[:, width:width + 1].astype(jnp.float32) - 1.0
    column = lax.broadcasted_iota(jnp.int32, (count, 3 * members), 1) % members
    chosen = flag(member == column.astype(jnp.float32)).astype(jnp.bfloat16)
    select[...] = chosen
    owner = lax.axis_index("owner")
    slab = block_of(width)
    for low in range(0, width, slab):
        here = pl.ds(low, slab)
        data = rows[:, here].astype(jnp.float32)
        for offset, result in ((0, gate_in), (width, up_in)):
            table = thirds(in_factors[owner, :, pl.ds(offset + low, slab)])
            scale = jnp.dot(chosen, table, preferred_element_type=jnp.float32)
            result[:, here] = (data * scale).astype(jnp.bfloat16)

    def one_block(step, first):
        @pl.when(step + SLOTS - 1 < steps)
        def _():
            for copy in arrivals(step + SLOTS - 1):
                copy.start()

        here = pl.ds(pl.multiple_of(step * block, block), block)
        chosen = select[...]
        gate_table = thirds(hid_factors[:, 0, here])
        up_table = thirds(hid_factors[:, 1, here])
        gate_scale = jnp.dot(chosen, gate_table, preferred_element_type=jnp.float32)
        up_scale = jnp.dot(chosen, up_table, preferred_element_type=jnp.float32)
        gate = jnp.dot(gate_in[...], gate_weight[:, here], preferred_element_type=jnp.float32)
        up_copy, down_copy = arrivals(step)
        up_copy.wait()
        up = jnp.dot(up_in[...], up_here[step % SLOTS], preferred_element_type=jnp.float32)
        gate = gate * gate_scale
        hidden = (gate / (1.0 + jnp.exp(-gate)) * (up * up_scale)).astype(jnp.bfloat16)
        down_copy.wait()
        part = jnp.dot(hidden, down_here[step % SLOTS], preferred_element_type=jnp.float32)
        total[...] = part if first else total[...] + part

    one_block(0, True)

    def body(step, carry):
        one_block(step, False)
        return carry

    lax.fori_loop(1, steps, body, 0)
    low = 0
    for result in results:
        result[...] = total[pl.ds(low, result.shape[0]), :].astype(jnp.bfloat16)
        low += result.shape[0]


def add_kernel(mine, other, *blocks):
    for spot, block in enumerate(blocks):
        here = pl.ds(spot * CAP, CAP)
        both = mine[here, :].astype(jnp.float32) + other[here, :].astype(jnp.float32)
        block[...] = both.astype(jnp.bfloat16)


def combine_kernel(ids, member_ids, weights, out_factors, *refs):
    mixed, summed = refs[-2:]
    for spot, block in enumerate(refs[:-2]):
        summed[pl.ds(spot * CAP, CAP), :] = block[...]
    tok_count = ids.shape[1]
    table = thirds(out_factors[...])
    entries = out_factors.shape[0]
    spot = lax.broadcasted_iota(jnp.int32, (3 * entries, tok_count), 0) % entries
    diagonal = lax.broadcasted_iota(jnp.int32, (tok_count, tok_count), 0) == (
        lax.broadcasted_iota(jnp.int32, (tok_count, tok_count), 1)
    )
    over_rows = (((0,), (0,)), ((), ()))
    result = None
    for route, place in enumerate(placing(ids[...])):
        picked = lax.dot_general(
            place.astype(jnp.bfloat16), summed[...], over_rows, preferred_element_type=jnp.float32
        )
        entry = ids[route:route + 1, :] * MEMBERS + member_ids[...]
        chosen = flag(spot == entry).astype(jnp.bfloat16)
        scale = lax.dot_general(chosen, table, over_rows, preferred_element_type=jnp.float32)
        weight = jnp.sum(
            jnp.where(diagonal, weights[route:route + 1, :], 0.0), axis=1, keepdims=True
        )
        term = picked * scale * weight
        result = term if result is None else result + term
    mixed[...] = result.astype(jnp.bfloat16)


def block_of(units):
    best = LANES
    for block in range(LANES, 513, LANES):
        if units % block == 0:
            best = block
    return best


def fetch_kernel(*refs):
    half = len(refs) // 2
    sources, results, arrived = refs[:half], refs[half:-1], refs[-1]
    copies = []
    for source, result in zip(sources, results):
        rows = source.shape[0] // CHUNKS
        for chunk in range(CHUNKS):
            part = pl.ds(chunk * rows, rows)
            copies.append(
                pltpu.make_async_copy(source.at[part], result.at[part], arrived.at[len(copies)])
            )
    for copy in copies:
        copy.start()
    for copy in copies:
        copy.wait()


def fetched(weights):
    vmem = pl.BlockSpec(memory_space=pltpu.VMEM)
    size = sum(weight.size * weight.dtype.itemsize for weight in weights)
    return pl.pallas_call(
        fetch_kernel,
        in_specs=[pl.BlockSpec(memory_space=pltpu.HBM)] * len(weights),
        out_specs=[vmem] * len(weights),
        out_shape=[jax.ShapeDtypeStruct(weight.shape, weight.dtype) for weight in weights],
        scratch_shapes=[pltpu.SemaphoreType.DMA((CHUNKS * len(weights),))],
        compiler_params=pltpu.CompilerParams(vmem_limit_bytes=VMEM_LARGE),
        cost_estimate=pl.CostEstimate(
            flops=512 * size, bytes_accessed=size, transcendentals=0
        ),
        name="fetch",
    )(*weights)


def run_rows(parts, sizes, gate_weight, up_weight, down_weight, input_factors, hidden_factors):
    count = sum(sizes)
    width, units = gate_weight.shape
    block = block_of(units)
    members = input_factors.shape[1]
    vmem = pl.BlockSpec(memory_space=pltpu.VMEM)
    hbm = pl.BlockSpec(memory_space=pltpu.HBM)
    return pl.pallas_call(
        ffn_kernel,
        in_specs=[vmem] * 3 + [hbm] * 2 + [vmem] * len(parts),
        out_specs=[vmem] * len(sizes),
        out_shape=[jax.ShapeDtypeStruct((size, width), jnp.bfloat16) for size in sizes],
        scratch_shapes=[
            pltpu.VMEM((count, width + LANES), jnp.bfloat16),
            pltpu.VMEM((count, width), jnp.bfloat16),
            pltpu.VMEM((count, width), jnp.bfloat16),
            pltpu.VMEM((count, 3 * members), jnp.bfloat16),
            pltpu.VMEM((count, width), jnp.float32),
            pltpu.VMEM((SLOTS, width, block), jnp.bfloat16),
            pltpu.VMEM((SLOTS, block, width), jnp.bfloat16),
            pltpu.SemaphoreType.DMA((2, SLOTS)),
        ],
        compiler_params=pltpu.CompilerParams(
            vmem_limit_bytes=VMEM_LARGE
        ),
        name="ffn",
    )(input_factors, hidden_factors, gate_weight, up_weight, down_weight, *parts)


def swapped(block, axis, apart):
    route = [(place, place ^ apart) for place in range(lax.axis_size(axis))]
    return lax.ppermute(block, axis, route)


def traded(blocks):
    last = len(blocks) - 1
    return [
        swapped(block, "owner", last - spot) if spot < last else block
        for spot, block in enumerate(blocks)
    ]


def per_device(
    tokens,
    expert_ids,
    member_ids,
    combine_weights,
    gate_weight,
    up_weight,
    down_weight,
    input_factors,
    hidden_factors,
    output_factors,
):
    split = lax.axis_size("share")
    levels = split.bit_length() - 1
    tok_count, width = tokens.shape
    slots = EXPERTS * CAP
    ids = expert_ids.T
    members = member_ids.reshape(1, tok_count)
    small = pltpu.CompilerParams(vmem_limit_bytes=VMEM_SPARE)
    blocks = pl.pallas_call(
        pack_kernel,
        out_shape=[jax.ShapeDtypeStruct((CAP, width + LANES), jnp.bfloat16)] * EXPERTS,
        compiler_params=small,
        name="pack",
    )(tokens, ids, members)
    *blocks, gate_weight = lax.optimization_barrier((*blocks, gate_weight))
    arrived = traded(blocks)
    *arrived, gate_weight = lax.optimization_barrier((*arrived, *fetched((gate_weight,))))
    groups = [[] for _ in range(levels + 1)]
    for block in arrived:
        held = [block]
        for level in range(levels):
            give = held[0] if level == 0 else jnp.concatenate(held, axis=0)
            held.append(swapped(give, "share", 1 << level))
        for group, part in zip(groups, held):
            group.append(part)
    parts = [part for group in groups for part in group]
    sizes = [sum(part.shape[0] for part in group) for group in groups]
    results = list(run_rows(
            parts, sizes, gate_weight, up_weight, down_weight, input_factors, hidden_factors
        ))
    for level in reversed(range(1, levels)):
        other = swapped(results.pop(), "share", 1 << level).reshape(EXPERTS, -1, width)
        low = 0
        for spot, mine in enumerate(results):
            rows = mine.shape[0] // EXPERTS
            theirs = other[:, low:low + rows].reshape(mine.shape)
            both = mine.astype(jnp.float32) + theirs.astype(jnp.float32)
            results[spot] = both.astype(jnp.bfloat16)
            low += rows
    blocks = pl.pallas_call(
        add_kernel,
        out_shape=[jax.ShapeDtypeStruct((CAP, width), jnp.bfloat16)] * EXPERTS,
        compiler_params=small,
        name="add",
    )(results[0], swapped(results[1], "share", 1))
    returned = traded(blocks)
    return pl.pallas_call(
        combine_kernel,
        out_shape=jax.ShapeDtypeStruct((tok_count, width), jnp.bfloat16),
        scratch_shapes=[pltpu.VMEM((slots, width), jnp.bfloat16)],
        compiler_params=small,
        name="combine",
    )(
        ids, members, combine_weights.T,
        output_factors.reshape(EXPERTS * MEMBERS, width), *returned,
    )


def solution(mesh):
    groups = mesh.shape["groups"]
    fine = Mesh(mesh.devices.reshape(groups, EXPERTS, -1), ("groups", "owner", "share"))
    expert = ("owner", "share")
    everyone = ("groups", "owner", "share")
    in_specs = (
        P(everyone, None),
        P(everyone, None),
        P(everyone),
        P(everyone, None),
        P(None, expert),
        P(None, expert),
        P(expert, None),
        P(),
        P(None, None, expert),
        P(),
    )
    return jax.shard_map(
        per_device, mesh=fine, in_specs=in_specs, out_specs=P(everyone, None), check_vma=False
    )
```

```python
import functools

import jax
import jax.numpy as jnp
from jax import lax
from jax.experimental import pallas as pl
from jax.experimental.pallas import tpu as pltpu
from jax.sharding import Mesh, PartitionSpec as P

EXPERTS = 8
MEMBERS = 8
CAP = 16
LANES = 128
VMEM_SPARE = 3 << 20
VMEM_LARGE = 36 << 20
SLOTS = 3
CHUNKS = 4


def thirds(table):
    high = table.astype(jnp.bfloat16)
    rest = table - high.astype(jnp.float32)
    middle = rest.astype(jnp.bfloat16)
    low = (rest - middle.astype(jnp.float32)).astype(jnp.bfloat16)
    return jnp.concatenate([high, middle, low], axis=0)


def flag(condition):
    return jnp.where(condition, 1.0, 0.0)


def placing(ids):
    tok_count = ids.shape[1]
    slots = EXPERTS * CAP
    row = lax.broadcasted_iota(jnp.int32, (slots, tok_count), 0)
    expert = (EXPERTS - 1 - row // CAP) ^ lax.axis_index("owner")
    first = ids[0:1, :] == expert
    second = ids[1:2, :] == expert
    named = flag(first) + flag(second)
    before = flag(
        lax.broadcasted_iota(jnp.int32, (tok_count, tok_count), 0)
        < lax.broadcasted_iota(jnp.int32, (tok_count, tok_count), 1)
    ).astype(jnp.bfloat16)
    rank = jnp.dot(named.astype(jnp.bfloat16), before, preferred_element_type=jnp.float32)
    here = rank == (row % CAP).astype(jnp.float32)
    return flag(first & here), flag(second & here)


def pack_kernel(tokens, ids, member_ids, *blocks):
    width = tokens.shape[1]
    first, second = placing(ids[...])
    chosen = first + second
    rows = jnp.dot(
        chosen.astype(jnp.bfloat16), tokens[...], preferred_element_type=jnp.float32
    ).astype(jnp.bfloat16)
    plus = (member_ids[...] + 1).astype(jnp.float32)
    member = jnp.sum(chosen * plus, axis=1, keepdims=True)
    member = jnp.broadcast_to(member, (rows.shape[0], LANES)).astype(jnp.bfloat16)
    for spot, block in enumerate(blocks):
        block[:, :width] = rows[spot * CAP:(spot + 1) * CAP]
        block[:, width:] = member[spot * CAP:(spot + 1) * CAP]


def ffn_kernel(in_factors, hid_factors, gate_weight, up_weight, down_weight, *refs):
    rows, gate_in, up_in, select, total, up_here, down_here, arrived = refs[-8:]
    count, width = gate_in.shape
    results, parts, low = [], list(refs[:-8]), 0
    while low < count:
        results.insert(0, parts.pop())
        low += results[0].shape[0]
    members = in_factors.shape[1]
    units = gate_weight.shape[1]
    block = block_of(units)
    steps = units // block

    def arrivals(step):
        here = pl.ds(step * block, block)
        slot = step % SLOTS
        return (
            pltpu.make_async_copy(up_weight.at[:, here], up_here.at[slot], arrived.at[0, slot]),
            pltpu.make_async_copy(down_weight.at[here], down_here.at[slot], arrived.at[1, slot]),
        )

    for step in range(min(SLOTS - 1, steps)):
        for copy in arrivals(step):
            copy.start()
    low = 0
    for part in parts:
        rows[pl.ds(low, part.shape[0]), :] = part[...]
        low += part.shape[0]
    member = rows[:, width:width + 1].astype(jnp.float32) - 1.0
    column = lax.broadcasted_iota(jnp.int32, (count, 3 * members), 1) % members
    chosen = flag(member == column.astype(jnp.float32)).astype(jnp.bfloat16)
    select[...] = chosen
    owner = lax.axis_index("owner")
    slab = block_of(width)
    for low in range(0, width, slab):
        here = pl.ds(low, slab)
        data = rows[:, here].astype(jnp.float32)
        for offset, result in ((0, gate_in), (width, up_in)):
            table = thirds(in_factors[owner, :, pl.ds(offset + low, slab)])
            scale = jnp.dot(chosen, table, preferred_element_type=jnp.float32)
            result[:, here] = (data * scale).astype(jnp.bfloat16)

    for step in range(steps):
        here = pl.ds(step * block, block)
        if step + SLOTS - 1 < steps:
            for copy in arrivals(step + SLOTS - 1):
                copy.start()
        chosen = select[...]
        gate_table = thirds(hid_factors[:, 0, here])
        up_table = thirds(hid_factors[:, 1, here])
        gate_scale = jnp.dot(chosen, gate_table, preferred_element_type=jnp.float32)
        up_scale = jnp.dot(chosen, up_table, preferred_element_type=jnp.float32)
        gate = jnp.dot(gate_in[...], gate_weight[:, here], preferred_element_type=jnp.float32)
        up_copy, down_copy = arrivals(step)
        up_copy.wait()
        up = jnp.dot(up_in[...], up_here[step % SLOTS], preferred_element_type=jnp.float32)
        gate = gate * gate_scale
        hidden = (gate / (1.0 + jnp.exp(-gate)) * (up * up_scale)).astype(jnp.bfloat16)
        down_copy.wait()
        part = jnp.dot(hidden, down_here[step % SLOTS], preferred_element_type=jnp.float32)
        total[...] = total[...] + part if step else part

    low = 0
    for result in results:
        result[...] = total[pl.ds(low, result.shape[0]), :].astype(jnp.bfloat16)
        low += result.shape[0]


def add_kernel(mine, other, *blocks):
    for spot, block in enumerate(blocks):
        here = pl.ds(spot * CAP, CAP)
        both = mine[here, :].astype(jnp.float32) + other[here, :].astype(jnp.float32)
        block[...] = both.astype(jnp.bfloat16)


def combine_kernel(ids, member_ids, weights, out_factors, *refs):
    mixed, summed = refs[-2:]
    for spot, block in enumerate(refs[:-2]):
        summed[pl.ds(spot * CAP, CAP), :] = block[...]
    tok_count = ids.shape[1]
    table = thirds(out_factors[...])
    entries = out_factors.shape[0]
    spot = lax.broadcasted_iota(jnp.int32, (3 * entries, tok_count), 0) % entries
    diagonal = lax.broadcasted_iota(jnp.int32, (tok_count, tok_count), 0) == (
        lax.broadcasted_iota(jnp.int32, (tok_count, tok_count), 1)
    )
    over_rows = (((0,), (0,)), ((), ()))
    result = None
    for route, place in enumerate(placing(ids[...])):
        picked = lax.dot_general(
            place.astype(jnp.bfloat16), summed[...], over_rows, preferred_element_type=jnp.float32
        )
        entry = ids[route:route + 1, :] * MEMBERS + member_ids[...]
        chosen = flag(spot == entry).astype(jnp.bfloat16)
        scale = lax.dot_general(chosen, table, over_rows, preferred_element_type=jnp.float32)
        weight = jnp.sum(
            jnp.where(diagonal, weights[route:route + 1, :], 0.0), axis=1, keepdims=True
        )
        term = picked * scale * weight
        result = term if result is None else result + term
    mixed[...] = result.astype(jnp.bfloat16)


def block_of(units):
    best = LANES
    for block in range(LANES, 513, LANES):
        if units % block == 0:
            best = block
    return best


def fetch_kernel(*refs):
    half = len(refs) // 2
    sources, results, arrived = refs[:half], refs[half:-1], refs[-1]
    copies = []
    for source, result in zip(sources, results):
        rows = source.shape[0] // CHUNKS
        for chunk in range(CHUNKS):
            part = pl.ds(chunk * rows, rows)
            copies.append(
                pltpu.make_async_copy(source.at[part], result.at[part], arrived.at[len(copies)])
            )
    for copy in copies:
        copy.start()
    for copy in copies:
        copy.wait()


def fetched(weights):
    vmem = pl.BlockSpec(memory_space=pltpu.VMEM)
    size = sum(weight.size * weight.dtype.itemsize for weight in weights)
    return pl.pallas_call(
        fetch_kernel,
        in_specs=[pl.BlockSpec(memory_space=pltpu.HBM)] * len(weights),
        out_specs=[vmem] * len(weights),
        out_shape=[jax.ShapeDtypeStruct(weight.shape, weight.dtype) for weight in weights],
        scratch_shapes=[pltpu.SemaphoreType.DMA((CHUNKS * len(weights),))],
        compiler_params=pltpu.CompilerParams(vmem_limit_bytes=VMEM_LARGE),
        cost_estimate=pl.CostEstimate(
            flops=512 * size, bytes_accessed=size, transcendentals=0
        ),
        name="fetch",
    )(*weights)


def run_rows(parts, sizes, gate_weight, up_weight, down_weight, input_factors, hidden_factors):
    count = sum(sizes)
    width, units = gate_weight.shape
    block = block_of(units)
    members = input_factors.shape[1]
    vmem = pl.BlockSpec(memory_space=pltpu.VMEM)
    hbm = pl.BlockSpec(memory_space=pltpu.HBM)
    return pl.pallas_call(
        ffn_kernel,
        in_specs=[vmem] * 3 + [hbm] * 2 + [vmem] * len(parts),
        out_specs=[vmem] * len(sizes),
        out_shape=[jax.ShapeDtypeStruct((size, width), jnp.bfloat16) for size in sizes],
        scratch_shapes=[
            pltpu.VMEM((count, width + LANES), jnp.bfloat16),
            pltpu.VMEM((count, width), jnp.bfloat16),
            pltpu.VMEM((count, width), jnp.bfloat16),
            pltpu.VMEM((count, 3 * members), jnp.bfloat16),
            pltpu.VMEM((count, width), jnp.float32),
            pltpu.VMEM((SLOTS, width, block), jnp.bfloat16),
            pltpu.VMEM((SLOTS, block, width), jnp.bfloat16),
            pltpu.SemaphoreType.DMA((2, SLOTS)),
        ],
        compiler_params=pltpu.CompilerParams(
            vmem_limit_bytes=VMEM_LARGE
        ),
        name="ffn",
    )(input_factors, hidden_factors, gate_weight, up_weight, down_weight, *parts)


def swapped(block, axis, apart):
    route = [(place, place ^ apart) for place in range(lax.axis_size(axis))]
    return lax.ppermute(block, axis, route)


def traded(blocks):
    last = len(blocks) - 1
    return [
        swapped(block, "owner", last - spot) if spot < last else block
        for spot, block in enumerate(blocks)
    ]


def per_device(
    tokens,
    expert_ids,
    member_ids,
    combine_weights,
    gate_weight,
    up_weight,
    down_weight,
    input_factors,
    hidden_factors,
    output_factors,
):
    split = lax.axis_size("share")
    levels = split.bit_length() - 1
    tok_count, width = tokens.shape
    slots = EXPERTS * CAP
    ids = expert_ids.T
    members = member_ids.reshape(1, tok_count)
    small = pltpu.CompilerParams(vmem_limit_bytes=VMEM_SPARE)
    blocks = pl.pallas_call(
        pack_kernel,
        out_shape=[jax.ShapeDtypeStruct((CAP, width + LANES), jnp.bfloat16)] * EXPERTS,
        compiler_params=small,
        name="pack",
    )(tokens, ids, members)
    *blocks, gate_weight = lax.optimization_barrier((*blocks, gate_weight))
    arrived = traded(blocks)
    *arrived, gate_weight = lax.optimization_barrier((*arrived, *fetched((gate_weight,))))
    groups = [[] for _ in range(levels + 1)]
    for block in arrived:
        held = [block]
        for level in range(levels):
            give = held[0] if level == 0 else jnp.concatenate(held, axis=0)
            held.append(swapped(give, "share", 1 << level))
        for group, part in zip(groups, held):
            group.append(part)
    parts = [part for group in groups for part in group]
    sizes = [sum(part.shape[0] for part in group) for group in groups]
    results = list(run_rows(
            parts, sizes, gate_weight, up_weight, down_weight, input_factors, hidden_factors
        ))
    for level in reversed(range(1, levels)):
        other = swapped(results.pop(), "share", 1 << level).reshape(EXPERTS, -1, width)
        low = 0
        for spot, mine in enumerate(results):
            rows = mine.shape[0] // EXPERTS
            theirs = other[:, low:low + rows].reshape(mine.shape)
            both = mine.astype(jnp.float32) + theirs.astype(jnp.float32)
            results[spot] = both.astype(jnp.bfloat16)
            low += rows
    blocks = pl.pallas_call(
        add_kernel,
        out_shape=[jax.ShapeDtypeStruct((CAP, width), jnp.bfloat16)] * EXPERTS,
        compiler_params=small,
        name="add",
    )(results[0], swapped(results[1], "share", 1))
    returned = traded(blocks)
    return pl.pallas_call(
        combine_kernel,
        out_shape=jax.ShapeDtypeStruct((tok_count, width), jnp.bfloat16),
        scratch_shapes=[pltpu.VMEM((slots, width), jnp.bfloat16)],
        compiler_params=small,
        name="combine",
    )(
        ids, members, combine_weights.T,
        output_factors.reshape(EXPERTS * MEMBERS, width), *returned,
    )


def solution(mesh):
    groups = mesh.shape["groups"]
    fine = Mesh(mesh.devices.reshape(groups, EXPERTS, -1), ("groups", "owner", "share"))
    expert = ("owner", "share")
    everyone = ("groups", "owner", "share")
    in_specs = (
        P(everyone, None),
        P(everyone, None),
        P(everyone),
        P(everyone, None),
        P(None, expert),
        P(None, expert),
        P(expert, None),
        P(),
        P(None, None, expert),
        P(),
    )
    return jax.shard_map(
        per_device, mesh=fine, in_specs=in_specs, out_specs=P(everyone, None), check_vma=False
    )
```

```python
import functools

import jax
import jax.numpy as jnp
from jax import lax
from jax.experimental import pallas as pl
from jax.experimental.pallas import tpu as pltpu
from jax.sharding import Mesh, PartitionSpec as P

EXPERTS = 8
MEMBERS = 8
CAP = 16
LANES = 128
VMEM_SPARE = 3 << 20
VMEM_LARGE = 36 << 20
SLOTS = 3
CHUNKS = 4


def thirds(table):
    high = table.astype(jnp.bfloat16)
    rest = table - high.astype(jnp.float32)
    middle = rest.astype(jnp.bfloat16)
    low = (rest - middle.astype(jnp.float32)).astype(jnp.bfloat16)
    return jnp.concatenate([high, middle, low], axis=0)


def flag(condition):
    return jnp.where(condition, 1.0, 0.0)


def placing(ids):
    tok_count = ids.shape[1]
    slots = EXPERTS * CAP
    row = lax.broadcasted_iota(jnp.int32, (slots, tok_count), 0)
    expert = (EXPERTS - 1 - row // CAP) ^ lax.axis_index("owner")
    first = ids[0:1, :] == expert
    second = ids[1:2, :] == expert
    named = flag(first) + flag(second)
    before = flag(
        lax.broadcasted_iota(jnp.int32, (tok_count, tok_count), 0)
        < lax.broadcasted_iota(jnp.int32, (tok_count, tok_count), 1)
    ).astype(jnp.bfloat16)
    rank = jnp.dot(named.astype(jnp.bfloat16), before, preferred_element_type=jnp.float32)
    here = rank == (row % CAP).astype(jnp.float32)
    return flag(first & here), flag(second & here)


def pack_kernel(tokens, ids, member_ids, *blocks):
    width = tokens.shape[1]
    first, second = placing(ids[...])
    chosen = first + second
    rows = jnp.dot(
        chosen.astype(jnp.bfloat16), tokens[...], preferred_element_type=jnp.float32
    ).astype(jnp.bfloat16)
    plus = (member_ids[...] + 1).astype(jnp.float32)
    member = jnp.sum(chosen * plus, axis=1, keepdims=True)
    member = jnp.broadcast_to(member, (rows.shape[0], LANES)).astype(jnp.bfloat16)
    for spot, block in enumerate(blocks):
        block[:, :width] = rows[spot * CAP:(spot + 1) * CAP]
        block[:, width:] = member[spot * CAP:(spot + 1) * CAP]


def ffn_kernel(in_factors, hid_factors, gate_weight, up_weight, down_weight, *refs):
    rows, gate_in, up_in, select, total, up_here, down_here, arrived = refs[-8:]
    count, width = gate_in.shape
    results, parts, low = [], list(refs[:-8]), 0
    while low < count:
        results.insert(0, parts.pop())
        low += results[0].shape[0]
    members = in_factors.shape[1]
    units = gate_weight.shape[1]
    block = block_of(units)
    steps = units // block

    def arrivals(step):
        here = pl.ds(step * block, block)
        slot = step % SLOTS
        return (
            pltpu.make_async_copy(up_weight.at[:, here], up_here.at[slot], arrived.at[0, slot]),
            pltpu.make_async_copy(down_weight.at[here], down_here.at[slot], arrived.at[1, slot]),
        )

    for step in range(min(SLOTS - 1, steps)):
        for copy in arrivals(step):
            copy.start()
    low = 0
    for part in parts:
        rows[pl.ds(low, part.shape[0]), :] = part[...]
        low += part.shape[0]
    member = rows[:, width:width + 1].astype(jnp.float32) - 1.0
    column = lax.broadcasted_iota(jnp.int32, (count, 3 * members), 1) % members
    chosen = flag(member == column.astype(jnp.float32)).astype(jnp.bfloat16)
    select[...] = chosen
    owner = lax.axis_index("owner")
    slab = block_of(width)
    for low in range(0, width, slab):
        here = pl.ds(low, slab)
        data = rows[:, here].astype(jnp.float32)
        for offset, result in ((0, gate_in), (width, up_in)):
            table = thirds(in_factors[owner, :, pl.ds(offset + low, slab)])
            scale = jnp.dot(chosen, table, preferred_element_type=jnp.float32)
            result[:, here] = (data * scale).astype(jnp.bfloat16)

    for step in range(steps):
        here = pl.ds(step * block, block)
        if step + SLOTS - 1 < steps:
            for copy in arrivals(step + SLOTS - 1):
                copy.start()
        chosen = select[...]
        gate_table = thirds(hid_factors[:, 0, here])
        up_table = thirds(hid_factors[:, 1, here])
        gate_scale = jnp.dot(chosen, gate_table, preferred_element_type=jnp.float32)
        up_scale = jnp.dot(chosen, up_table, preferred_element_type=jnp.float32)
        gate = jnp.dot(gate_in[...], gate_weight[:, here], preferred_element_type=jnp.float32)
        up_copy, down_copy = arrivals(step)
        up_copy.wait()
        up = jnp.dot(up_in[...], up_here[step % SLOTS], preferred_element_type=jnp.float32)
        gate = gate * gate_scale
        hidden = (gate / (1.0 + jnp.exp(-gate)) * (up * up_scale)).astype(jnp.bfloat16)
        down_copy.wait()
        part = jnp.dot(hidden, down_here[step % SLOTS], preferred_element_type=jnp.float32)
        total[...] = total[...] + part if step else part

    low = 0
    for result in results:
        result[...] = total[pl.ds(low, result.shape[0]), :].astype(jnp.bfloat16)
        low += result.shape[0]


def add_kernel(mine, other, *blocks):
    for spot, block in enumerate(blocks):
        here = pl.ds(spot * CAP, CAP)
        both = mine[here, :].astype(jnp.float32) + other[here, :].astype(jnp.float32)
        block[...] = both.astype(jnp.bfloat16)


def scale_kernel(ids, member_ids, weights, out_factors, scales):
    tok_count = ids.shape[1]
    table = thirds(out_factors[...])
    entries = out_factors.shape[0]
    spot = lax.broadcasted_iota(jnp.int32, (3 * entries, tok_count), 0) % entries
    diagonal = lax.broadcasted_iota(jnp.int32, (tok_count, tok_count), 0) == (
        lax.broadcasted_iota(jnp.int32, (tok_count, tok_count), 1)
    )
    for route in range(2):
        entry = ids[route:route + 1, :] * MEMBERS + member_ids[...]
        chosen = flag(spot == entry).astype(jnp.bfloat16)
        scale = lax.dot_general(
            chosen, table, (((0,), (0,)), ((), ())), preferred_element_type=jnp.float32
        )
        weight = jnp.sum(
            jnp.where(diagonal, weights[route:route + 1, :], 0.0), axis=1, keepdims=True
        )
        scales[route] = scale * weight


def combine_kernel(ids, scales, *refs):
    mixed, summed = refs[-2:]
    for spot, block in enumerate(refs[:-2]):
        summed[pl.ds(spot * CAP, CAP), :] = block[...]
    result = None
    for route, place in enumerate(placing(ids[...])):
        picked = lax.dot_general(
            place.astype(jnp.bfloat16), summed[...], (((0,), (0,)), ((), ())),
            preferred_element_type=jnp.float32,
        )
        term = picked * scales[route]
        result = term if result is None else result + term
    mixed[...] = result.astype(jnp.bfloat16)


def block_of(units):
    best = LANES
    for block in range(LANES, 513, LANES):
        if units % block == 0:
            best = block
    return best


def fetch_kernel(*refs):
    half = len(refs) // 2
    sources, results, arrived = refs[:half], refs[half:-1], refs[-1]
    copies = []
    for source, result in zip(sources, results):
        rows = source.shape[0] // CHUNKS
        for chunk in range(CHUNKS):
            part = pl.ds(chunk * rows, rows)
            copies.append(
                pltpu.make_async_copy(source.at[part], result.at[part], arrived.at[len(copies)])
            )
    for copy in copies:
        copy.start()
    for copy in copies:
        copy.wait()


def fetched(weights):
    vmem = pl.BlockSpec(memory_space=pltpu.VMEM)
    size = sum(weight.size * weight.dtype.itemsize for weight in weights)
    return pl.pallas_call(
        fetch_kernel,
        in_specs=[pl.BlockSpec(memory_space=pltpu.HBM)] * len(weights),
        out_specs=[vmem] * len(weights),
        out_shape=[jax.ShapeDtypeStruct(weight.shape, weight.dtype) for weight in weights],
        scratch_shapes=[pltpu.SemaphoreType.DMA((CHUNKS * len(weights),))],
        compiler_params=pltpu.CompilerParams(vmem_limit_bytes=VMEM_LARGE),
        cost_estimate=pl.CostEstimate(
            flops=512 * size, bytes_accessed=size, transcendentals=0
        ),
        name="fetch",
    )(*weights)


def run_rows(parts, sizes, gate_weight, up_weight, down_weight, input_factors, hidden_factors):
    count = sum(sizes)
    width, units = gate_weight.shape
    block = block_of(units)
    members = input_factors.shape[1]
    vmem = pl.BlockSpec(memory_space=pltpu.VMEM)
    hbm = pl.BlockSpec(memory_space=pltpu.HBM)
    return pl.pallas_call(
        ffn_kernel,
        in_specs=[vmem] * 3 + [hbm] * 2 + [vmem] * len(parts),
        out_specs=[vmem] * len(sizes),
        out_shape=[jax.ShapeDtypeStruct((size, width), jnp.bfloat16) for size in sizes],
        scratch_shapes=[
            pltpu.VMEM((count, width + LANES), jnp.bfloat16),
            pltpu.VMEM((count, width), jnp.bfloat16),
            pltpu.VMEM((count, width), jnp.bfloat16),
            pltpu.VMEM((count, 3 * members), jnp.bfloat16),
            pltpu.VMEM((count, width), jnp.float32),
            pltpu.VMEM((SLOTS, width, block), jnp.bfloat16),
            pltpu.VMEM((SLOTS, block, width), jnp.bfloat16),
            pltpu.SemaphoreType.DMA((2, SLOTS)),
        ],
        compiler_params=pltpu.CompilerParams(
            vmem_limit_bytes=VMEM_LARGE
        ),
        name="ffn",
    )(input_factors, hidden_factors, gate_weight, up_weight, down_weight, *parts)


def swapped(block, axis, apart):
    route = [(place, place ^ apart) for place in range(lax.axis_size(axis))]
    return lax.ppermute(block, axis, route)


def traded(blocks):
    last = len(blocks) - 1
    return [
        swapped(block, "owner", last - spot) if spot < last else block
        for spot, block in enumerate(blocks)
    ]


def per_device(
    tokens,
    expert_ids,
    member_ids,
    combine_weights,
    gate_weight,
    up_weight,
    down_weight,
    input_factors,
    hidden_factors,
    output_factors,
):
    split = lax.axis_size("share")
    levels = split.bit_length() - 1
    tok_count, width = tokens.shape
    slots = EXPERTS * CAP
    ids = expert_ids.T
    members = member_ids.reshape(1, tok_count)
    small = pltpu.CompilerParams(vmem_limit_bytes=VMEM_SPARE)
    blocks = pl.pallas_call(
        pack_kernel,
        out_shape=[jax.ShapeDtypeStruct((CAP, width + LANES), jnp.bfloat16)] * EXPERTS,
        compiler_params=small,
        name="pack",
    )(tokens, ids, members)
    *blocks, gate_weight = lax.optimization_barrier((*blocks, gate_weight))
    arrived = traded(blocks)
    *arrived, own = arrived
    *arrived, gate_weight = lax.optimization_barrier((*arrived, *fetched((gate_weight,))))
    arrived.append(own)
    groups = [[] for _ in range(levels + 1)]
    for block in arrived:
        held = [block]
        for level in range(levels):
            give = held[0] if level == 0 else jnp.concatenate(held, axis=0)
            held.append(swapped(give, "share", 1 << level))
        for group, part in zip(groups, held):
            group.append(part)
    parts = [part for group in groups for part in group]
    sizes = [sum(part.shape[0] for part in group) for group in groups]
    results = list(run_rows(
            parts, sizes, gate_weight, up_weight, down_weight, input_factors, hidden_factors
        ))
    for level in reversed(range(1, levels)):
        other = swapped(results.pop(), "share", 1 << level).reshape(EXPERTS, -1, width)
        low = 0
        for spot, mine in enumerate(results):
            rows = mine.shape[0] // EXPERTS
            theirs = other[:, low:low + rows].reshape(mine.shape)
            both = mine.astype(jnp.float32) + theirs.astype(jnp.float32)
            results[spot] = both.astype(jnp.bfloat16)
            low += rows
    blocks = pl.pallas_call(
        add_kernel,
        out_shape=[jax.ShapeDtypeStruct((CAP, width), jnp.bfloat16)] * EXPERTS,
        compiler_params=small,
        name="add",
    )(results[0], swapped(results[1], "share", 1))
    scales = pl.pallas_call(
        scale_kernel,
        out_shape=jax.ShapeDtypeStruct((2, tok_count, width), jnp.float32),
        compiler_params=small,
        cost_estimate=pl.CostEstimate(
            flops=1 << 30, bytes_accessed=4 * output_factors.size, transcendentals=0
        ),
        name="scale",
    )(ids, members, combine_weights.T, output_factors.reshape(EXPERTS * MEMBERS, width))
    returned = traded(blocks)
    return pl.pallas_call(
        combine_kernel,
        out_shape=jax.ShapeDtypeStruct((tok_count, width), jnp.bfloat16),
        scratch_shapes=[pltpu.VMEM((slots, width), jnp.bfloat16)],
        compiler_params=small,
        name="combine",
    )(ids, scales, *returned)


def solution(mesh):
    groups = mesh.shape["groups"]
    fine = Mesh(mesh.devices.reshape(groups, EXPERTS, -1), ("groups", "owner", "share"))
    expert = ("owner", "share")
    everyone = ("groups", "owner", "share")
    in_specs = (
        P(everyone, None),
        P(everyone, None),
        P(everyone),
        P(everyone, None),
        P(None, expert),
        P(None, expert),
        P(expert, None),
        P(),
        P(None, None, expert),
        P(),
    )
    return jax.shard_map(
        per_device, mesh=fine, in_specs=in_specs, out_specs=P(everyone, None), check_vma=False
    )
```

```python
import functools

import jax
import jax.numpy as jnp
from jax import lax
from jax.experimental import pallas as pl
from jax.experimental.pallas import tpu as pltpu
from jax.sharding import Mesh, PartitionSpec as P

EXPERTS = 8
MEMBERS = 8
CAP = 16
LANES = 128
VMEM_SPARE = 3 << 20
VMEM_LARGE = 36 << 20
SLOTS = 3
CHUNKS = 4


def thirds(table):
    high = table.astype(jnp.bfloat16)
    rest = table - high.astype(jnp.float32)
    middle = rest.astype(jnp.bfloat16)
    low = (rest - middle.astype(jnp.float32)).astype(jnp.bfloat16)
    return jnp.concatenate([high, middle, low], axis=0)


def flag(condition):
    return jnp.where(condition, 1.0, 0.0)


def placing(ids):
    tok_count = ids.shape[1]
    slots = EXPERTS * CAP
    row = lax.broadcasted_iota(jnp.int32, (slots, tok_count), 0)
    expert = (EXPERTS - 1 - row // CAP) ^ lax.axis_index("owner")
    first = ids[0:1, :] == expert
    second = ids[1:2, :] == expert
    named = flag(first) + flag(second)
    before = flag(
        lax.broadcasted_iota(jnp.int32, (tok_count, tok_count), 0)
        < lax.broadcasted_iota(jnp.int32, (tok_count, tok_count), 1)
    ).astype(jnp.bfloat16)
    rank = jnp.dot(named.astype(jnp.bfloat16), before, preferred_element_type=jnp.float32)
    here = rank == (row % CAP).astype(jnp.float32)
    return flag(first & here), flag(second & here)


def pack_kernel(tokens, ids, member_ids, *blocks):
    width = tokens.shape[1]
    first, second = placing(ids[...])
    chosen = first + second
    rows = jnp.dot(
        chosen.astype(jnp.bfloat16), tokens[...], preferred_element_type=jnp.float32
    ).astype(jnp.bfloat16)
    plus = (member_ids[...] + 1).astype(jnp.float32)
    member = jnp.sum(chosen * plus, axis=1, keepdims=True)
    member = jnp.broadcast_to(member, (rows.shape[0], LANES)).astype(jnp.bfloat16)
    for spot, block in enumerate(blocks):
        block[:, :width] = rows[spot * CAP:(spot + 1) * CAP]
        block[:, width:] = member[spot * CAP:(spot + 1) * CAP]


def ffn_kernel(in_factors, hid_factors, gate_weight, up_weight, down_weight, *refs):
    rows, gate_in, up_in, select, total, up_here, down_here, arrived = refs[-8:]
    count, width = gate_in.shape
    results, parts, low = [], list(refs[:-8]), 0
    while low < count:
        results.insert(0, parts.pop())
        low += results[0].shape[0]
    members = in_factors.shape[1]
    units = gate_weight.shape[1]
    block = block_of(units)
    steps = units // block

    def arrivals(step):
        here = pl.ds(step * block, block)
        slot = step % SLOTS
        return (
            pltpu.make_async_copy(up_weight.at[:, here], up_here.at[slot], arrived.at[0, slot]),
            pltpu.make_async_copy(down_weight.at[here], down_here.at[slot], arrived.at[1, slot]),
        )

    for step in range(min(SLOTS - 1, steps)):
        for copy in arrivals(step):
            copy.start()
    low = 0
    for part in parts:
        rows[pl.ds(low, part.shape[0]), :] = part[...]
        low += part.shape[0]
    member = rows[:, width:width + 1].astype(jnp.float32) - 1.0
    column = lax.broadcasted_iota(jnp.int32, (count, 3 * members), 1) % members
    chosen = flag(member == column.astype(jnp.float32)).astype(jnp.bfloat16)
    select[...] = chosen
    owner = lax.axis_index("owner")
    slab = block_of(width)
    for low in range(0, width, slab):
        here = pl.ds(low, slab)
        data = rows[:, here].astype(jnp.float32)
        for offset, result in ((0, gate_in), (width, up_in)):
            table = thirds(in_factors[owner, :, pl.ds(offset + low, slab)])
            scale = jnp.dot(chosen, table, preferred_element_type=jnp.float32)
            result[:, here] = (data * scale).astype(jnp.bfloat16)

    for step in range(steps):
        here = pl.ds(step * block, block)
        if step + SLOTS - 1 < steps:
            for copy in arrivals(step + SLOTS - 1):
                copy.start()
        chosen = select[...]
        gate_table = thirds(hid_factors[:, 0, here])
        up_table = thirds(hid_factors[:, 1, here])
        gate_scale = jnp.dot(chosen, gate_table, preferred_element_type=jnp.float32)
        up_scale = jnp.dot(chosen, up_table, preferred_element_type=jnp.float32)
        gate = jnp.dot(gate_in[...], gate_weight[:, here], preferred_element_type=jnp.float32)
        up_copy, down_copy = arrivals(step)
        up_copy.wait()
        up = jnp.dot(up_in[...], up_here[step % SLOTS], preferred_element_type=jnp.float32)
        gate = gate * gate_scale
        hidden = (gate / (1.0 + jnp.exp(-gate)) * (up * up_scale)).astype(jnp.bfloat16)
        down_copy.wait()
        part = jnp.dot(hidden, down_here[step % SLOTS], preferred_element_type=jnp.float32)
        total[...] = total[...] + part if step else part

    low = 0
    for result in results:
        result[...] = total[pl.ds(low, result.shape[0]), :].astype(jnp.bfloat16)
        low += result.shape[0]


def gather_kernel(*refs):
    for spot, block in enumerate(refs[:-1]):
        refs[-1][pl.ds(spot * CAP, CAP), :] = block[...]


def add_kernel(mine, other, *blocks):
    for spot, block in enumerate(blocks):
        here = pl.ds(spot * CAP, CAP)
        both = mine[here, :].astype(jnp.float32) + other[here, :].astype(jnp.float32)
        block[...] = both.astype(jnp.bfloat16)


def scale_kernel(ids, member_ids, weights, out_factors, scales):
    tok_count = ids.shape[1]
    table = thirds(out_factors[...])
    entries = out_factors.shape[0]
    spot = lax.broadcasted_iota(jnp.int32, (3 * entries, tok_count), 0) % entries
    diagonal = lax.broadcasted_iota(jnp.int32, (tok_count, tok_count), 0) == (
        lax.broadcasted_iota(jnp.int32, (tok_count, tok_count), 1)
    )
    for route in range(2):
        entry = ids[route:route + 1, :] * MEMBERS + member_ids[...]
        chosen = flag(spot == entry).astype(jnp.bfloat16)
        scale = lax.dot_general(
            chosen, table, (((0,), (0,)), ((), ())), preferred_element_type=jnp.float32
        )
        weight = jnp.sum(
            jnp.where(diagonal, weights[route:route + 1, :], 0.0), axis=1, keepdims=True
        )
        scales[route] = scale * weight


def combine_kernel(ids, scales, *refs):
    mixed, summed = refs[-2:]
    for spot, block in enumerate(refs[:-2]):
        summed[pl.ds(spot * CAP, CAP), :] = block[...]
    result = None
    for route, place in enumerate(placing(ids[...])):
        picked = lax.dot_general(
            place.astype(jnp.bfloat16), summed[...], (((0,), (0,)), ((), ())),
            preferred_element_type=jnp.float32,
        )
        term = picked * scales[route]
        result = term if result is None else result + term
    mixed[...] = result.astype(jnp.bfloat16)


def block_of(units):
    best = LANES
    for block in range(LANES, 513, LANES):
        if units % block == 0:
            best = block
    return best


def fetch_kernel(*refs):
    half = len(refs) // 2
    sources, results, arrived = refs[:half], refs[half:-1], refs[-1]
    copies = []
    for source, result in zip(sources, results):
        rows = source.shape[0] // CHUNKS
        for chunk in range(CHUNKS):
            part = pl.ds(chunk * rows, rows)
            copies.append(
                pltpu.make_async_copy(source.at[part], result.at[part], arrived.at[len(copies)])
            )
    for copy in copies:
        copy.start()
    for copy in copies:
        copy.wait()


def fetched(weights):
    vmem = pl.BlockSpec(memory_space=pltpu.VMEM)
    size = sum(weight.size * weight.dtype.itemsize for weight in weights)
    return pl.pallas_call(
        fetch_kernel,
        in_specs=[pl.BlockSpec(memory_space=pltpu.HBM)] * len(weights),
        out_specs=[vmem] * len(weights),
        out_shape=[jax.ShapeDtypeStruct(weight.shape, weight.dtype) for weight in weights],
        scratch_shapes=[pltpu.SemaphoreType.DMA((CHUNKS * len(weights),))],
        compiler_params=pltpu.CompilerParams(vmem_limit_bytes=VMEM_LARGE),
        cost_estimate=pl.CostEstimate(
            flops=512 * size, bytes_accessed=size, transcendentals=0
        ),
        name="fetch",
    )(*weights)


def run_rows(parts, sizes, gate_weight, up_weight, down_weight, input_factors, hidden_factors):
    count = sum(sizes)
    width, units = gate_weight.shape
    block = block_of(units)
    members = input_factors.shape[1]
    vmem = pl.BlockSpec(memory_space=pltpu.VMEM)
    hbm = pl.BlockSpec(memory_space=pltpu.HBM)
    return pl.pallas_call(
        ffn_kernel,
        in_specs=[vmem] * 3 + [hbm] * 2 + [vmem] * len(parts),
        out_specs=[vmem] * len(sizes),
        out_shape=[jax.ShapeDtypeStruct((size, width), jnp.bfloat16) for size in sizes],
        scratch_shapes=[
            pltpu.VMEM((count, width + LANES), jnp.bfloat16),
            pltpu.VMEM((count, width), jnp.bfloat16),
            pltpu.VMEM((count, width), jnp.bfloat16),
            pltpu.VMEM((count, 3 * members), jnp.bfloat16),
            pltpu.VMEM((count, width), jnp.float32),
            pltpu.VMEM((SLOTS, width, block), jnp.bfloat16),
            pltpu.VMEM((SLOTS, block, width), jnp.bfloat16),
            pltpu.SemaphoreType.DMA((2, SLOTS)),
        ],
        compiler_params=pltpu.CompilerParams(
            vmem_limit_bytes=VMEM_LARGE
        ),
        name="ffn",
    )(input_factors, hidden_factors, gate_weight, up_weight, down_weight, *parts)


def swapped(block, axis, apart):
    route = [(place, place ^ apart) for place in range(lax.axis_size(axis))]
    return lax.ppermute(block, axis, route)


def traded(blocks):
    last = len(blocks) - 1
    return [
        swapped(block, "owner", last - spot) if spot < last else block
        for spot, block in enumerate(blocks)
    ]


def per_device(
    tokens,
    expert_ids,
    member_ids,
    combine_weights,
    gate_weight,
    up_weight,
    down_weight,
    input_factors,
    hidden_factors,
    output_factors,
):
    split = lax.axis_size("share")
    levels = split.bit_length() - 1
    tok_count, width = tokens.shape
    slots = EXPERTS * CAP
    ids = expert_ids.T
    members = member_ids.reshape(1, tok_count)
    small = pltpu.CompilerParams(vmem_limit_bytes=VMEM_SPARE)
    blocks = pl.pallas_call(
        pack_kernel,
        out_shape=[jax.ShapeDtypeStruct((CAP, width + LANES), jnp.bfloat16)] * EXPERTS,
        compiler_params=small,
        name="pack",
    )(tokens, ids, members)
    *blocks, gate_weight = lax.optimization_barrier((*blocks, gate_weight))
    arrived = traded(blocks)
    *arrived, gate_weight = lax.optimization_barrier((*arrived, *fetched((gate_weight,))))
    parts = [
        pl.pallas_call(
            gather_kernel,
            out_shape=jax.ShapeDtypeStruct((slots, width + LANES), jnp.bfloat16),
            compiler_params=small,
            name="gather",
        )(*arrived)
    ]
    for level in range(levels):
        give = parts[0] if level == 0 else jnp.concatenate(parts, axis=0)
        parts.append(swapped(give, "share", 1 << level))
    sizes = [part.shape[0] for part in parts]
    results = list(run_rows(
            parts, sizes, gate_weight, up_weight, down_weight, input_factors, hidden_factors
        ))
    for level in reversed(range(1, levels)):
        other = swapped(results.pop(), "share", 1 << level).astype(jnp.float32)
        low = 0
        for spot, mine in enumerate(results):
            high = low + mine.shape[0]
            results[spot] = (mine.astype(jnp.float32) + other[low:high]).astype(jnp.bfloat16)
            low = high
    blocks = pl.pallas_call(
        add_kernel,
        out_shape=[jax.ShapeDtypeStruct((CAP, width), jnp.bfloat16)] * EXPERTS,
        compiler_params=small,
        name="add",
    )(results[0], swapped(results[1], "share", 1))
    scales = pl.pallas_call(
        scale_kernel,
        out_shape=jax.ShapeDtypeStruct((2, tok_count, width), jnp.float32),
        compiler_params=small,
        cost_estimate=pl.CostEstimate(
            flops=1 << 30, bytes_accessed=4 * output_factors.size, transcendentals=0
        ),
        name="scale",
    )(ids, members, combine_weights.T, output_factors.reshape(EXPERTS * MEMBERS, width))
    returned = traded(blocks)
    return pl.pallas_call(
        combine_kernel,
        out_shape=jax.ShapeDtypeStruct((tok_count, width), jnp.bfloat16),
        scratch_shapes=[pltpu.VMEM((slots, width), jnp.bfloat16)],
        compiler_params=small,
        name="combine",
    )(ids, scales, *returned)


def solution(mesh):
    groups = mesh.shape["groups"]
    fine = Mesh(mesh.devices.reshape(groups, EXPERTS, -1), ("groups", "owner", "share"))
    expert = ("owner", "share")
    everyone = ("groups", "owner", "share")
    in_specs = (
        P(everyone, None),
        P(everyone, None),
        P(everyone),
        P(everyone, None),
        P(None, expert),
        P(None, expert),
        P(expert, None),
        P(),
        P(None, None, expert),
        P(),
    )
    return jax.shard_map(
        per_device, mesh=fine, in_specs=in_specs, out_specs=P(everyone, None), check_vma=False
    )
```
